32 devices in a mesh: lag: 16 (over z, y, x), row: 2 (over core).
Axes of the slice: x: 2, y: 2, z: 4, core: 2. Of those that a mesh axis runs over, the one named last changes fastest.
Arguments:
- blocks: bfloat16 [32, 2048, 2048], P('lag', 'row'), may hold values from -0.03125 to 0.03125
- history: bfloat16 [32, 2048, 128], P('lag'), may hold values from -6 to 6
- excitation: float32 [2, 2048, 128], P(None, 'row'), may hold values from -6 to 6
- self_inverse: float32 [2048, 2048], P('lag', 'row'), may hold values from -2 to 2
Outputs:
- currents: float32 [2, 2048, 128], P(None, 'lag')
The draws below stay inside these ranges and needn't reach their ends.
All inputs are finite; a program needn't handle non-finite values.
Results may differ from the reference program's by a relative error of at most 0.0003.
Values may be sent and summed in bfloat16 or wider, within the bound.
A program may use at most 64 MiB of HBM per device.

```python
import math
import jax
import jax.numpy as jnp
from jax import lax

P_SIZE = 2048
COLUMNS = 128
STEPS = 2
LAGS = 32


def draw_self_inverse(key, part):
    first, second = jax.random.split(jax.random.fold_in(key, 11))
    diagonal = jnp.exp(jax.random.uniform(first, (P_SIZE,), jnp.float32, math.log(0.5), math.log(1.8)))
    spread = jnp.clip(jax.random.normal(second, (P_SIZE, P_SIZE), jnp.float32), -4.0, 4.0)
    return spread * (0.6 / math.sqrt(P_SIZE)) + jnp.diag(diagonal)


def spiked(drawn, own_key, source, target, shards_of, factor):
    owner, partner = [(jnp.arange(drawn.shape[position]) // (drawn.shape[position] // shards_of)).reshape([-1 if axis == position else 1 for axis in range(drawn.ndim)]) for position in (source, target)]
    chosen = jax.random.permutation(own_key, shards_of)[partner]
    strong = (owner == chosen) | (owner == (partner + shards_of // 2) % shards_of)
    return jnp.where(strong, factor * drawn, drawn)


def level_of(rng, dims, shards, least, largest):
    def one(dim, shards_of):
        draws = jax.random.uniform(jax.random.fold_in(jax.random.fold_in(rng, 6), dim), (shards_of,), jnp.float32, least / len(shards), largest / len(shards))
        return jnp.repeat(jnp.exp(draws), dims[dim] // shards_of).reshape((-1,) + (1,) * (len(dims) - dim - 1))

    factor_of = one(*shards[0])
    for cut in shards[1:]:
        factor_of = factor_of * one(*cut)
    return factor_of


def gaussian(stream_key, shape, deviation, bound, cuts=(), held_as=jnp.bfloat16):
    entries = deviation * jax.random.normal(stream_key, shape, jnp.float32)
    if cuts:
        entries = entries * level_of(stream_key, shape, cuts, -0.22, 0.18)
    return jnp.clip(entries, -bound, bound).astype(held_as)


def gaussian_with(stream_key, extent, scale, bound, pieces, heavy, kind=jnp.bfloat16):
    result = scale * jax.random.normal(stream_key, extent, jnp.float32)
    if pieces:
        result = result * level_of(stream_key, extent, pieces, -0.22, 0.18)
    return jnp.clip(spiked(result, jax.random.fold_in(stream_key, 3), *heavy), -bound, bound).astype(kind)


def setup_inputs(seed: int = 0) -> dict:
    key_of = jax.random.split(jax.random.key(seed), 5)
    return {
        "blocks": gaussian_with(key_of[0], (LAGS, P_SIZE, P_SIZE), (P_SIZE * LAGS) ** -0.5, 0.03125, ((0, 16), (1, 2)), (0, 1, 16, 2.0)),
        "history": gaussian(key_of[1], (LAGS, P_SIZE, COLUMNS), 1.0, 6.0, ((0, 16),)),
        "excitation": gaussian(key_of[2], (STEPS, P_SIZE, COLUMNS), 1.0, 6.0, ((1, 2),), jnp.float32),
        "self_inverse": draw_self_inverse(jax.random.fold_in(key_of[4], 71), 0),
    }


def lag_total(blocks, past):
    def add_lag(total, pair):
        return total + jnp.dot(pair[0], pair[1], preferred_element_type=jnp.float32), None

    start = jnp.zeros((blocks.shape[1], past.shape[2]), jnp.float32)
    return lax.scan(add_lag, start, (blocks, past))[0]


def reference(blocks, history, excitation, self_inverse):
    past = history
    results = []
    for marker in range(STEPS):
        summed = lag_total(blocks, past)
        residual = excitation[marker] - summed
        current = jnp.dot(self_inverse, residual, precision=lax.Precision.HIGHEST, preferred_element_type=jnp.float32)
        results.append(current)
        past = jnp.concatenate([current.astype(jnp.bfloat16)[None], past[:-1]], axis=0)
    return jnp.stack(results)
```

```python
import functools

import jax
import jax.numpy as jnp
from jax import lax
from jax.experimental import pallas as pl
from jax.experimental.pallas import tpu as pltpu
from jax.sharding import PartitionSpec as P

F32 = jnp.float32
BF16 = jnp.bfloat16


def split_of(lags):
    outer = 1
    while outer * outer * 4 <= lags and lags % (outer * 2) == 0:
        outer *= 2
    return outer, lags // outer


def kernel(A, B, R, G, blocks, history, excitation, inverse, out, *scratch):
    (bvm, hist, hprev, exc, inv, pbuf, rs1, mid, rs2, ag, ex, cbuf, gbuf, dbuf, dpiece, ld, ldb, hs, hr, hds, hdr,
     s1, r1, s2, r2, zs, zr, xs, xr, es, er, gs, gr, gds, gdr, ds, dr) = scratch
    L = A * B
    nloc = hist.shape[0]
    s, C = ag.shape[2], ag.shape[3]
    rows = A * s
    i = lax.axis_index("lag")
    r = lax.axis_index("row")
    a, b = i // B, lax.rem(i, B)
    mine = b * A + a

    def at(lag, row):
        return {"lag": lag, "row": row}

    def plane(k):
        return at(a * B + lax.rem(b + k, B), r)

    def line(k):
        return at(lax.rem(a + k, A) * B + b, r)

    def beside(k):
        return at(i, lax.rem(r + k, R))

    def put(src, dst, ss, rs, to):
        c = pltpu.make_async_remote_copy(src_ref=src, dst_ref=dst, send_sem=ss, recv_sem=rs, device_id=to, device_id_type=pl.DeviceIdType.MESH)
        c.start()
        return c

    def got(dst, ss, rs, to):
        pltpu.make_async_remote_copy(src_ref=dst, dst_ref=dst, send_sem=ss, recv_sem=rs, device_id=to, device_id_type=pl.DeviceIdType.MESH).wait_recv()

    hcopy = pltpu.make_async_copy(history, hist, ld.at[0])
    hcopy.start()
    loads = []
    for k in range(1, B + 1):
        g = pl.multiple_of(lax.rem(b + k, B) * rows, rows)
        c = pltpu.make_async_copy(blocks.at[:, pl.ds(g, rows)], bvm.at[:, pl.ds(g, rows)], ldb.at[k - 1])
        c.start()
        loads.append(c)
    ecopy = pltpu.make_async_copy(excitation.at[:, mine], exc, ld.at[1])
    ecopy.start()
    icopy = pltpu.make_async_copy(inverse, inv, ld.at[2])
    icopy.start()

    barrier = pltpu.get_barrier_semaphore()

    def hello(to):
        pl.semaphore_signal(barrier, inc=1, device_id=to, device_id_type=pl.DeviceIdType.MESH)

    for k in range(1, B):
        hello(plane(k))
    for k in range(1, A):
        hello(line(k))
    for k in range(1, R):
        hello(beside(k))

    @pl.when(i > 0)
    def _():
        hello(at(i - 1, r))
        hello(at(0, r))

    @pl.when(i < L - 1)
    def _():
        hello(at(i + 1, r))

    @pl.when(i == 0)
    def _():
        for j in range(1, L):
            hello(at(j, r))

    root, last = 1 - (i + L - 1) // L, (i + 1) // L
    pl.semaphore_wait(barrier, A + B + R - 3 + 2 * (1 - root) + (1 - last) + (L - 1) * root)

    sends = []

    def scatter_first(t, operand_of, before):
        for k in range(1, B + 1):
            before(k)
            to = lax.rem(b + k, B)
            g = pl.multiple_of(to * rows, rows)
            total = jnp.dot(bvm[0, pl.ds(g, rows), :], operand_of(0), preferred_element_type=F32)
            for l in range(1, nloc):
                total += jnp.dot(bvm[l, pl.ds(g, rows), :], operand_of(l), preferred_element_type=F32)
            for n in range(A):
                pbuf[t, to, n] = total[n * s:(n + 1) * s]
            if k < B:
                sends.append(put(pbuf.at[t, to], rs1.at[t, k - 1], s1.at[t, k - 1], r1.at[t, k - 1], plane(k)))

    def scatter_second(t):
        for k in range(1, B):
            got(rs1.at[t, k - 1], s1.at[t, k - 1], r1.at[t, k - 1], plane(k))
        for k in range(1, A + 1):
            to = lax.rem(a + k, A)
            total = pbuf[t, b, to]
            for n in range(B - 1):
                total += rs1[t, n, to]
            mid[t, k - 1] = total
            if k < A:
                sends.append(put(mid.at[t, k - 1], rs2.at[t, k - 1], s2.at[t, k - 1], r2.at[t, k - 1], line(k)))
        total = mid[t, A - 1]
        for k in range(1, A):
            got(rs2.at[t, k - 1], s2.at[t, k - 1], r2.at[t, k - 1], line(k))
            total += rs2[t, k - 1]
        return total

    def gather(t):
        for k in range(1, A):
            sends.append(put(ag.at[t, mine], ag.at[t, mine], zs.at[t, k - 1], zr.at[t, k - 1], line(k)))

        def spread(n):
            piece = b * A + lax.rem(a + A - n, A)
            if n:
                got(ag.at[t, piece], zs.at[t, n - 1], zr.at[t, n - 1], line(n))
            for k in range(1, B):
                sends.append(put(ag.at[t, piece], ag.at[t, piece], xs.at[t, n, k - 1], xr.at[t, n, k - 1], plane(k)))

        for n in range(A):
            spread(n)
        for n in range(A):
            for k in range(1, B):
                piece = lax.rem(b + B - k, B) * A + lax.rem(a + A - n, A)
                got(ag.at[t, piece], xs.at[t, n, k - 1], xr.at[t, n, k - 1], plane(k))

    def solve(t):
        full = ag[t].reshape(L * s, C)
        ex[t, r] = jnp.dot(inv[...], full, precision=lax.Precision.HIGHEST, preferred_element_type=F32)
        for k in range(1, R):
            sends.append(put(ex.at[t, r], ex.at[t, r], es.at[t, k - 1], er.at[t, k - 1], beside(k)))
        for k in range(1, R):
            got(ex.at[t, lax.rem(r + R - k, R)], es.at[t, k - 1], er.at[t, k - 1], beside(k))
        total = ex[t, 0]
        for n in range(1, R):
            total += ex[t, n]
        out[t] = total
        return total

    def before(k):
        if k == 1:
            hcopy.wait()
        loads[k - 1].wait()

    scatter_first(0, lambda l: hist[l], before)
    part = hprev.shape[0] // R
    share = pl.ds(pl.multiple_of(r * part, part), part)

    @pl.when(i < L - 1)
    def _():
        put(hist.at[nloc - 1, share], hprev.at[share], hs.at[0], hr.at[0], at(i + 1, r))

    ecopy.wait()
    icopy.wait()
    ag[0, mine] = exc[0] - scatter_second(0)
    gather(0)
    current = solve(0).astype(BF16)
    h = cbuf.shape[1]
    for n in range(G):
        cbuf[n] = current[n * h:(n + 1) * h]
    which = r if G > 1 else 0

    @pl.when(i > 0)
    def _():
        put(cbuf.at[which], gbuf.at[i, which], gs.at[0], gr.at[i], at(0, r))

    @pl.when(i > 0)
    def _():
        got(hprev.at[share], hs.at[0], hr.at[0], at(i - 1, r))

    @pl.when(i == 0)
    def _():
        hprev[...] = jnp.zeros_like(hprev)

    @pl.when(i > 0)
    def _():
        for k in range(1, R):
            put(hprev.at[share], hprev.at[share], hds.at[k - 1], hdr.at[k - 1], beside(k))
        for k in range(1, R):
            theirs = pl.ds(pl.multiple_of(lax.rem(r + R - k, R) * part, part), part)
            got(hprev.at[theirs], hds.at[k - 1], hdr.at[k - 1], beside(k))

    scatter_first(1, lambda l: hist[l - 1] if l else hprev[...], lambda k: None)

    @pl.when(i == 0)
    def _():
        gbuf[0, which] = cbuf[which]
        for j in range(1, L):
            got(gbuf.at[j, which], gs.at[0], gr.at[j], at(j, r))
        if G > 1:
            swaps = [put(gbuf.at[:, r], gbuf.at[:, r], gds.at[k - 1], gdr.at[k - 1], beside(k)) for k in range(1, R)]
            for k in range(1, R):
                got(gbuf.at[:, lax.rem(r + R - k, R)], gds.at[k - 1], gdr.at[k - 1], beside(k))
        newest = gbuf[...].reshape(L * G * h, C)
        for n in range(B):
            late = jnp.dot(bvm[0, n * rows:(n + 1) * rows, :], newest, preferred_element_type=F32)
            for m in range(A):
                dbuf[n * A + m] = late[m * s:(m + 1) * s]
                j = m * B + n
                if j:
                    put(dbuf.at[n * A + m], dpiece, ds.at[j], dr.at[0], at(j, r))
        dpiece[...] = dbuf[0]
        for j in range(1, L):
            pltpu.make_async_remote_copy(src_ref=dpiece, dst_ref=dpiece, send_sem=ds.at[j], recv_sem=dr.at[0], device_id=at(j, r), device_id_type=pl.DeviceIdType.MESH).wait_send()
        if G > 1:
            for c in swaps:
                c.wait_send()

    given = exc[1] - scatter_second(1)

    @pl.when(i > 0)
    def _():
        got(dpiece, ds.at[0], dr.at[0], at(0, r))

    ag[1, mine] = given - dpiece[...]
    gather(1)
    solve(1)

    for c in sends:
        c.wait_send()

    def left(src, ss, rs, to):
        pltpu.make_async_remote_copy(src_ref=src, dst_ref=src, send_sem=ss, recv_sem=rs, device_id=to, device_id_type=pl.DeviceIdType.MESH).wait_send()

    @pl.when(i < L - 1)
    def _():
        left(hprev.at[share], hs.at[0], hr.at[0], at(i + 1, r))

    @pl.when(i > 0)
    def _():
        left(cbuf.at[which], gs.at[0], gr.at[0], at(0, r))
        for k in range(1, R):
            left(hprev.at[share], hds.at[k - 1], hdr.at[k - 1], beside(k))


def solution(mesh):
    L, R = mesh.shape["lag"], mesh.shape["row"]
    A, B = split_of(L)

    def shards(blocks, history, excitation, inverse):
        nloc, pr, p = blocks.shape
        steps, _, C = excitation.shape
        q = inverse.shape[0]
        s = pr // L
        G = R if (q // R) % 16 == 0 else 1
        dma = pltpu.SemaphoreType.DMA
        return pl.pallas_call(
            functools.partial(kernel, A, B, R, G),
            out_shape=jax.ShapeDtypeStruct((steps, q, C), F32),
            in_specs=[pl.BlockSpec(memory_space=pl.ANY)] * 4,
            out_specs=pl.BlockSpec(memory_space=pltpu.VMEM),
            scratch_shapes=[
                pltpu.VMEM((nloc, pr, p), BF16),
                pltpu.VMEM((nloc, p, C), BF16),
                pltpu.VMEM((p, C), BF16),
                pltpu.VMEM((steps, s, C), F32),
                pltpu.VMEM((q, pr), F32),
                pltpu.VMEM((steps, B, A, s, C), F32),
                pltpu.VMEM((steps, B - 1, A, s, C), F32),
                pltpu.VMEM((steps, A, s, C), F32),
                pltpu.VMEM((steps, A - 1, s, C), F32),
                pltpu.VMEM((steps, L, s, C), F32),
                pltpu.VMEM((steps, R, q, C), F32),
                pltpu.VMEM((G, q // G, C), BF16),
                pltpu.VMEM((L, G, q // G, C), BF16),
                pltpu.VMEM((L, s, C), F32),
                pltpu.VMEM((s, C), F32),
                dma((3,)), dma((B,)), dma((1,)), dma((1,)), dma((R - 1,)), dma((R - 1,)),
                dma((steps, B - 1)), dma((steps, B - 1)), dma((steps, A - 1)), dma((steps, A - 1)),
                dma((steps, A - 1)), dma((steps, A - 1)), dma((steps, A, B - 1)), dma((steps, A, B - 1)),
                dma((steps, R - 1)), dma((steps, R - 1)),
                dma((1,)), dma((L,)), dma((R - 1,)), dma((R - 1,)), dma((L,)), dma((1,)),
            ],
            compiler_params=pltpu.CompilerParams(collective_id=0, has_side_effects=True, vmem_limit_bytes=60 * 1024 * 1024),
        )(blocks, history, excitation.reshape(steps, L, s, C), inverse)

    return jax.shard_map(
        shards,
        mesh=mesh,
        in_specs=(P("lag", "row", None), P("lag", None, None), P(None, "row", None), P("lag", "row")),
        out_specs=P(None, "lag", None),
        check_vma=False,
    )
```

```python
import functools

import jax
import jax.numpy as jnp
from jax import lax
from jax.experimental import pallas as pl
from jax.experimental.pallas import tpu as pltpu
from jax.sharding import PartitionSpec as P

F32 = jnp.float32
BF16 = jnp.bfloat16


def split_of(lags):
    outer = 1
    while outer * outer * 4 <= lags and lags % (outer * 2) == 0:
        outer *= 2
    return outer, lags // outer


def kernel(A, B, R, G, blocks, history, excitation, inverse, out, *scratch):
    (bvm, hist, exc, inv, pbuf, rs1, mid, rs2, ag, ex, cbuf, gbuf, dbuf, dpiece, ld, ldb, hs, hr, hds, hdr,
     s1, r1, s2, r2, zs, zr, xs, xr, es, er, gs, gr, gds, gdr, ds, dr) = scratch
    L = A * B
    nloc = bvm.shape[0]
    hprev = hist.at[0]
    s, C = ag.shape[2], ag.shape[3]
    rows = A * s
    i = lax.axis_index("lag")
    r = lax.axis_index("row")
    a, b = i // B, lax.rem(i, B)
    mine = b * A + a

    def at(lag, row):
        return {"lag": lag, "row": row}

    def flipped(k):
        place, step = b, 1
        while step < B:
            place = place + (k // step % 2) * (step - 2 * step * lax.rem(b // step, 2))
            step *= 2
        return place

    def plane(k):
        return at(a * B + flipped(k), r)

    def line(k):
        return at(lax.rem(a + k, A) * B + b, r)

    def beside(k):
        return at(i, lax.rem(r + k, R))

    def put(src, dst, ss, rs, to):
        c = pltpu.make_async_remote_copy(src_ref=src, dst_ref=dst, send_sem=ss, recv_sem=rs, device_id=to, device_id_type=pl.DeviceIdType.MESH)
        c.start()
        return c

    def got(dst, ss, rs, to):
        pltpu.make_async_remote_copy(src_ref=dst, dst_ref=dst, send_sem=ss, recv_sem=rs, device_id=to, device_id_type=pl.DeviceIdType.MESH).wait_recv()

    hcopy = pltpu.make_async_copy(history, hist.at[pl.ds(1, nloc)], ld.at[0])
    hcopy.start()
    for k in range(B - 1, -1, -1):
        g = pl.multiple_of(flipped(k) * rows, rows)
        c = pltpu.make_async_copy(blocks.at[:, pl.ds(g, rows)], bvm.at[:, pl.ds(g, rows)], ldb.at[k])
        c.start()
    ecopy = pltpu.make_async_copy(excitation.at[:, mine], exc, ld.at[1])
    ecopy.start()
    icopy = pltpu.make_async_copy(inverse, inv, ld.at[2])
    icopy.start()

    barrier = pltpu.get_barrier_semaphore()

    def hello(to):
        pl.semaphore_signal(barrier, inc=1, device_id=to, device_id_type=pl.DeviceIdType.MESH)

    for k in range(1, B):
        hello(plane(k))
    for k in range(1, A):
        hello(line(k))
    for k in range(1, R):
        hello(beside(k))

    @pl.when(i > 0)
    def _():
        hello(at(i - 1, r))
        hello(at(0, r))

    @pl.when(i < L - 1)
    def _():
        hello(at(i + 1, r))

    @pl.when(i == 0)
    def _():
        for j in range(1, L):
            hello(at(j, r))

    sends = []
    root, last = 1 - (i + L - 1) // L, (i + 1) // L
    pl.semaphore_wait(barrier, A + B + R - 3 + 2 * (1 - root) + (1 - last) + (L - 1) * root)


    def scatter_first(t, before):
        @pl.loop(0, B)
        def _(step):
            k = B - 1 - step
            before(k)
            to = flipped(k)
            g = pl.multiple_of(to * rows, rows)
            total = jnp.dot(bvm[0, pl.ds(g, rows), :], hist[1 - t], preferred_element_type=F32)
            for l in range(1, nloc):
                total += jnp.dot(bvm[l, pl.ds(g, rows), :], hist[l + 1 - t], preferred_element_type=F32)
            for n in range(A):
                pbuf[t, to, n] = total[n * s:(n + 1) * s]

            @pl.when(k > 0)
            def _():
                @pl.loop(1, A + 1)
                def _(m):
                    n = lax.rem(a + m, A)
                    put(pbuf.at[t, to, n], rs1.at[t, k - 1, n], s1.at[t, k - 1, m - 1], r1.at[t, k - 1, n], plane(k))

    def scatter_second(t):
        for k in range(1, A + 1):
            to = lax.rem(a + k, A)
            for n in range(B - 1, 0, -1):
                got(rs1.at[t, n - 1, to], s1.at[t, n - 1, k - 1], r1.at[t, n - 1, to], plane(n))
            total = pbuf[t, b, to]
            for n in range(B - 1):
                total += rs1[t, n, to]
            mid[t, k - 1] = total
            if k < A:
                sends.append(put(mid.at[t, k - 1], rs2.at[t, k - 1], s2.at[t, k - 1], r2.at[t, k - 1], line(k)))
        total = mid[t, A - 1]
        for k in range(1, A):
            got(rs2.at[t, k - 1], s2.at[t, k - 1], r2.at[t, k - 1], line(k))
            total += rs2[t, k - 1]
        return total

    def gather(t, between):
        for k in range(1, A):
            sends.append(put(ag.at[t, mine], ag.at[t, mine], zs.at[t, k - 1], zr.at[t, k - 1], line(k)))

        def piece_of(k, n):
            return flipped(k) * A + lax.rem(a + A - n, A)

        def spread(n, ks):
            piece = piece_of(0, n)
            for k in ks:
                sends.append(put(ag.at[t, piece], ag.at[t, piece], xs.at[t, n, k - 1], xr.at[t, n, k - 1], plane(k)))

        near = [k for k in range(1, B) if k & (k - 1) == 0]
        far = [k for k in range(1, B) if k & (k - 1)]
        spread(0, near + far)
        for n in range(1, A):
            got(ag.at[t, piece_of(0, n)], zs.at[t, n - 1], zr.at[t, n - 1], line(n))
            spread(n, near)
        for n in range(1, A):
            spread(n, far)
        between()
        total = None
        for k in [0] + near + far:
            if k:
                for n in range(A):
                    got(ag.at[t, piece_of(k, n)], xs.at[t, n, k - 1], xr.at[t, n, k - 1], plane(k))
            if rows % 128 == 0:
                g = pl.multiple_of(flipped(k) * rows, rows)
                term = exact(inv[:, pl.ds(g, rows)], ag[t, pl.ds(flipped(k) * A, A)].reshape(rows, C))
                total = term if total is None else total + term
        if total is None:
            total = exact(inv[...], ag[t].reshape(L * s, C))
        return total

    def exact(left, right):
        return jnp.dot(left, right, precision=lax.Precision.HIGHEST, preferred_element_type=F32)

    def solve(t, between):
        ex[t, r] = gather(t, between)
        for k in range(1, R):
            sends.append(put(ex.at[t, r], ex.at[t, r], es.at[t, k - 1], er.at[t, k - 1], beside(k)))
        for k in range(1, R):
            got(ex.at[t, lax.rem(r + R - k, R)], es.at[t, k - 1], er.at[t, k - 1], beside(k))
        total = ex[t, 0]
        for n in range(1, R):
            total += ex[t, n]
        out[t] = total
        return total

    hcopy.wait()

    def before(k):
        g = pl.multiple_of(flipped(k) * rows, rows)
        pltpu.make_async_copy(blocks.at[:, pl.ds(g, rows)], bvm.at[:, pl.ds(g, rows)], ldb.at[k]).wait()

    scatter_first(0, before)
    part = hist.shape[1] // R
    share = pl.ds(pl.multiple_of(r * part, part), part)

    @pl.when(i < L - 1)
    def _():
        put(hist.at[nloc, share], hprev.at[share], hs.at[0], hr.at[0], at(i + 1, r))

    def given_history():
        @pl.when(i > 0)
        def _():
            got(hprev.at[share], hs.at[0], hr.at[0], at(i - 1, r))

        @pl.when(i == 0)
        def _():
            hprev[...] = jnp.zeros(hist.shape[1:], BF16)

        @pl.when(i > 0)
        def _():
            for k in range(1, R):
                put(hprev.at[share], hprev.at[share], hds.at[k - 1], hdr.at[k - 1], beside(k))
            for k in range(1, R):
                theirs = pl.ds(pl.multiple_of(lax.rem(r + R - k, R) * part, part), part)
                got(hprev.at[theirs], hds.at[k - 1], hdr.at[k - 1], beside(k))

        scatter_first(1, lambda k: None)

    ecopy.wait()
    icopy.wait()
    ag[0, mine] = exc[0] - scatter_second(0)
    current = solve(0, given_history).astype(BF16)
    h = cbuf.shape[1]
    for n in range(G):
        cbuf[n] = current[n * h:(n + 1) * h]
    which = r if G > 1 else 0

    @pl.when(i > 0)
    def _():
        put(cbuf.at[which], gbuf.at[i, which], gs.at[0], gr.at[i], at(0, r))

    @pl.when(i == 0)
    def _():
        gbuf[0, which] = cbuf[which]
        swaps = []

        def swap(j):
            if G > 1:
                for k in range(1, R):
                    swaps.append(put(gbuf.at[j, r], gbuf.at[j, r], gds.at[k - 1, j], gdr.at[k - 1, j], beside(k)))

        swap(0)
        for j in range(1, L):
            got(gbuf.at[j, which], gs.at[0], gr.at[j], at(j, r))
            swap(j)
        if G > 1:
            for j in range(L):
                for k in range(1, R):
                    got(gbuf.at[j, lax.rem(r + R - k, R)], gds.at[k - 1, j], gdr.at[k - 1, j], beside(k))
        hist[0] = gbuf[...].reshape(L * G * h, C)

        @pl.loop(0, B)
        def _(n):
            late = jnp.dot(bvm[0, pl.ds(pl.multiple_of(n * rows, rows), rows), :], hist[0], preferred_element_type=F32)
            for m in range(A):
                dbuf[n * A + m] = late[m * s:(m + 1) * s]

            @pl.loop(0, A)
            def _(m):
                j = m * B + n

                @pl.when(j > 0)
                def _():
                    put(dbuf.at[n * A + m], dpiece, ds.at[j], dr.at[0], at(j, r))

        dpiece[...] = dbuf[0]
        for j in range(1, L):
            pltpu.make_async_remote_copy(src_ref=dpiece, dst_ref=dpiece, send_sem=ds.at[j], recv_sem=dr.at[0], device_id=at(j, r), device_id_type=pl.DeviceIdType.MESH).wait_send()
        for c in swaps:
            c.wait_send()

    given = exc[1] - scatter_second(1)

    @pl.when(i > 0)
    def _():
        got(dpiece, ds.at[0], dr.at[0], at(0, r))

    ag[1, mine] = given - dpiece[...]
    solve(1, lambda: None)

    def left(src, ss, rs, to):
        pltpu.make_async_remote_copy(src_ref=src, dst_ref=src, send_sem=ss, recv_sem=rs, device_id=to, device_id_type=pl.DeviceIdType.MESH).wait_send()

    @pl.loop(0, A)
    def _(m):
        for t in range(2):
            for k in range(1, B):
                n = lax.rem(a + m + 1, A)
                left(pbuf.at[t, flipped(k), n], s1.at[t, k - 1, m], r1.at[t, k - 1, n], plane(k))

    for c in sends:
        c.wait_send()

    @pl.when(i < L - 1)
    def _():
        left(hprev.at[share], hs.at[0], hr.at[0], at(i + 1, r))

    @pl.when(i > 0)
    def _():
        left(cbuf.at[which], gs.at[0], gr.at[0], at(0, r))
        for k in range(1, R):
            left(hprev.at[share], hds.at[k - 1], hdr.at[k - 1], beside(k))


def solution(mesh):
    L, R = mesh.shape["lag"], mesh.shape["row"]
    A, B = split_of(L)

    def shards(blocks, history, excitation, inverse):
        nloc, pr, p = blocks.shape
        steps, _, C = excitation.shape
        q = inverse.shape[0]
        s = pr // L
        G = R if (q // R) % 16 == 0 else 1
        dma = pltpu.SemaphoreType.DMA
        return pl.pallas_call(
            functools.partial(kernel, A, B, R, G),
            out_shape=jax.ShapeDtypeStruct((steps, q, C), F32),
            in_specs=[pl.BlockSpec(memory_space=pl.ANY)] * 4,
            out_specs=pl.BlockSpec(memory_space=pltpu.VMEM),
            scratch_shapes=[
                pltpu.VMEM((nloc, pr, p), BF16),
                pltpu.VMEM((nloc + 1, p, C), BF16),
                pltpu.VMEM((steps, s, C), F32),
                pltpu.VMEM((q, pr), F32),
                pltpu.VMEM((steps, B, A, s, C), F32),
                pltpu.VMEM((steps, B - 1, A, s, C), F32),
                pltpu.VMEM((steps, A, s, C), F32),
                pltpu.VMEM((steps, A - 1, s, C), F32),
                pltpu.VMEM((steps, L, s, C), F32),
                pltpu.VMEM((steps, R, q, C), F32),
                pltpu.VMEM((G, q // G, C), BF16),
                pltpu.VMEM((L, G, q // G, C), BF16),
                pltpu.VMEM((L, s, C), F32),
                pltpu.VMEM((s, C), F32),
                dma((3,)), dma((B,)), dma((1,)), dma((1,)), dma((R - 1,)), dma((R - 1,)),
                dma((steps, B - 1, A)), dma((steps, B - 1, A)), dma((steps, A - 1)), dma((steps, A - 1)),
                dma((steps, A - 1)), dma((steps, A - 1)), dma((steps, A, B - 1)), dma((steps, A, B - 1)),
                dma((steps, R - 1)), dma((steps, R - 1)),
                dma((1,)), dma((L,)), dma((R - 1, L)), dma((R - 1, L)), dma((L,)), dma((1,)),
            ],
            compiler_params=pltpu.CompilerParams(collective_id=0, has_side_effects=True, vmem_limit_bytes=60 * 1024 * 1024),
        )(blocks, history, excitation.reshape(steps, L, s, C), inverse)

    return jax.shard_map(
        shards,
        mesh=mesh,
        in_specs=(P("lag", "row", None), P("lag", None, None), P(None, "row", None), P("lag", "row")),
        out_specs=P(None, "lag", None),
        check_vma=False,
    )
```
